32 devices in a mesh: outer: 8 (over y, x, core), span: 4 (over z).
Axes of the slice: x: 2, y: 2, z: 4, core: 2. Of those that a mesh axis runs over, the one named last changes fastest.
Arguments:
- queries_in: bfloat16 [16, 2048, 16, 128], P('outer', 'span'), may hold values from -6 to 6
- keys_in: bfloat16 [16, 2048, 16, 128], P('outer', 'span'), may hold values from -6 to 6
- values_in: bfloat16 [16, 2048, 16, 128], P('outer', 'span'), may hold values from -6 to 6
- gate_rows: bfloat16 [16, 2048, 16, 128], P('outer', 'span'), may hold values from -6 to 6
- out_weight: bfloat16 [2048, 2048], P('outer'), may hold values from -0.125 to 0.125
Outputs:
- mixer_out: bfloat16 [16, 2048, 2048], P('outer', 'span')
The draws below stay inside these ranges and needn't reach their ends.
All inputs are finite; a program needn't handle non-finite values.
Results may differ from the reference program's by a relative error of at most 0.0023.
Values may be sent and summed in bfloat16 or wider, within the bound.
A program may use at most 256 MiB of HBM per device.

```python
import jax
import jax.numpy as jnp
from jax import lax

HEADS = 16
HEAD_SIZE = 128
BATCH = 16
TOKENS = 2048
WIDTH = 2048


def block_scale(own_key, dims, shards, low, largest):
    def one(position, parts):
        heights = jax.random.uniform(jax.random.fold_in(jax.random.fold_in(own_key, 6), position), (parts,), jnp.float32, low / len(shards), largest / len(shards))
        return jnp.repeat(jnp.exp(heights), dims[position] // parts).reshape((-1,) + (1,) * (len(dims) - position - 1))

    factor_of = one(*shards[0])
    for cut in shards[1:]:
        factor_of = factor_of * one(*cut)
    return factor_of


def scatter_about(own_key, dims, deviation, reach, shards=(), kind=jnp.bfloat16):
    entries = deviation * jax.random.normal(own_key, dims, jnp.float32)
    if shards:
        entries = entries * block_scale(own_key, dims, shards, -0.22, 0.18)
    return jnp.clip(entries, -reach, reach).astype(kind)


def setup_inputs(seed: int = 0) -> dict:
    streams_of = jax.random.split(jax.random.key(seed), 6)
    return {
        "queries_in": scatter_about(streams_of[0], (BATCH, TOKENS, HEADS, HEAD_SIZE), 1.0, 6.0, ((0, 8), (1, 4))),
        "keys_in": scatter_about(streams_of[1], (BATCH, TOKENS, HEADS, HEAD_SIZE), 1.0, 6.0, ((0, 8), (1, 4))),
        "values_in": scatter_about(streams_of[2], (BATCH, TOKENS, HEADS, HEAD_SIZE), 1.0, 6.0, ((0, 8), (1, 4))),
        "gate_rows": scatter_about(streams_of[3], (BATCH, TOKENS, HEADS, HEAD_SIZE), 1.0, 6.0, ((0, 8), (1, 4))),
        "out_weight": scatter_about(streams_of[4], (WIDTH, WIDTH), WIDTH ** -0.5, 0.125, ((0, 8),)),
    }


def feature_map(values):
    wide = values.astype(jnp.float32)
    return (jnp.where(wide > 0.0, wide + 1.0, jnp.exp(jnp.minimum(wide, 0.0)))).astype(jnp.bfloat16)


def close_heads(read, gate_rows, count):
    result = read * count ** 0.5
    result = result * jax.nn.sigmoid(gate_rows.astype(jnp.float32))
    return result.astype(jnp.bfloat16)


def ask_state(features, state, mass):
    small = lax.optimization_barrier(state.astype(jnp.bfloat16))
    top = jnp.einsum("bthd,bhde->bthe", features.astype(jnp.float32), small.astype(jnp.float32))
    bottom = jnp.einsum("bthd,bhd->bth", features.astype(jnp.float32), mass, precision=lax.Precision.HIGHEST)
    return top / (bottom + 1e-3)[..., None]


def reference(queries_in, keys_in, values_in, gate_rows, out_weight):
    query_feature, key_feature = lax.optimization_barrier((feature_map(queries_in), feature_map(keys_in)))
    state = jnp.einsum("bthd,bthe->bhde", key_feature.astype(jnp.float32), values_in.astype(jnp.float32)) / TOKENS
    mass = jnp.sum(key_feature.astype(jnp.float32), axis=1) / TOKENS
    mixed = close_heads(ask_state(query_feature, state, mass), gate_rows, TOKENS).reshape(BATCH, TOKENS, WIDTH)
    mixed = lax.optimization_barrier(mixed)
    mixer_out = jnp.einsum("btw,wv->btv", mixed.astype(jnp.float32), out_weight.astype(jnp.float32)).astype(jnp.bfloat16)
    return mixer_out
```

```python
import functools

import jax
import jax.numpy as jnp
from jax import lax
from jax.experimental import pallas as pl
from jax.experimental.pallas import tpu as pltpu
from jax.sharding import PartitionSpec as P

MESH = pl.DeviceIdType.MESH
TILE = 64
ROWS = 128


def feature_map(values):
    wide = values.astype(jnp.float32)
    return jnp.where(wide > 0.0, wide + 1.0, jnp.exp(jnp.minimum(wide, 0.0))).astype(jnp.bfloat16)


def kernel(
    no, ns, q_hbm, k_hbm, v_hbm, g_hbm, w_hbm, mixed_hbm, wfull,
    kin, vin, qin, gin, wown, kf, vt, qf, gs, part, acc, rr, rl, sr, sl, full, mown, mrecv, mixed,
    in_sem, w_sem, out_sem, wsend, wrecv, rr_send, rr_recv, rl_send, rl_recv,
    ag_sr, ag_sl, ag_recv, m_send, m_recv,
):
    batch, tokens, heads, size = q_hbm.shape
    depth = w_hbm.shape[0]
    half = depth // 2
    chunk = heads // ns
    count = tokens * ns
    o = lax.axis_index("outer")
    s = lax.axis_index("span")

    def remote(src, dst, send, recv, **where):
        return pltpu.make_async_remote_copy(
            src_ref=src, dst_ref=dst, send_sem=send, recv_sem=recv, device_id=where, device_id_type=MESH
        )

    own_w = pltpu.make_async_copy(w_hbm, wown, w_sem.at[0])
    own_w.start()
    loads = {}
    for b in range(batch):
        for n, (src, dst) in enumerate(((k_hbm, kin), (v_hbm, vin))):
            loads[n, b] = pltpu.make_async_copy(src.at[b], dst.at[b], in_sem.at[n, b])
            loads[n, b].start()
    for b in range(batch):
        for n, (src, dst) in enumerate(((q_hbm, qin), (g_hbm, gin))):
            loads[n + 2, b] = pltpu.make_async_copy(src.at[b], dst.at[b], in_sem.at[n + 2, b])
            loads[n + 2, b].start()

    grid = no == 8
    dc, dx, dy = 1 - 2 * (o % 2), 2 - 4 * ((o // 2) % 2), 4 - 8 * ((o // 4) % 2)
    if grid:
        partners = [o + dc, o + dx, o + dy]
    else:
        partners = [(o + d) % no for d in range(1, no)]
    barrier = pltpu.get_barrier_semaphore()
    for other in partners:
        pl.semaphore_signal(barrier, inc=1, device_id={"outer": other}, device_id_type=MESH)
    for d in range(1, ns):
        pl.semaphore_signal(barrier, inc=1, device_id={"span": (s + d) % ns}, device_id_type=MESH)
    pl.semaphore_wait(barrier, len(partners) + ns - 1)

    def rows(block, part_of=None):
        if part_of is None:
            return wfull.at[pl.ds(pl.multiple_of(block * depth, depth), depth)]
        return wfull.at[pl.ds(pl.multiple_of(block * depth + part_of * half, half), half)]

    own_w.wait()
    keep_w = pltpu.make_async_copy(wown, rows(o), w_sem.at[1])
    keep_w.start()
    sends = []

    def w_copy(n, src, dst, other):
        copy = remote(src, dst, wsend.at[n], wrecv.at[n], outer=other)
        copy.start()
        sends.append(copy)

    def w_take(n, dst, other):
        remote(dst, dst, wsend.at[n], wrecv.at[n], outer=other).wait_recv()

    if grid:
        xn, yn, pn = o + dx, o + dy, o + dc
        for n, other, h in ((0, xn, 0), (3, yn, 1), (1, xn, 1), (2, yn, 0)):
            w_copy(n, wown.at[pl.ds(h * half, half)], rows(o, h), other)
        w_copy(6, wown, rows(o), pn)
    else:
        for d in range(1, no):
            w_copy(d, wown, rows(o), (o + d) % no)

    def weights_a():
        if grid:
            w_take(0, rows(xn, 0), xn)
            w_copy(4, rows(xn, 0), rows(xn, 0), yn)
            w_copy(7, rows(xn, 0), rows(xn, 0), pn)
            w_take(3, rows(yn, 1), yn)
            w_copy(5, rows(yn, 1), rows(yn, 1), xn)
            w_copy(8, rows(yn, 1), rows(yn, 1), pn)

    def weights_b():
        if grid:
            w_take(1, rows(xn, 1), xn)
            w_copy(9, rows(xn, 1), rows(xn, 1), pn)
            w_take(2, rows(yn, 0), yn)
            w_copy(10, rows(yn, 0), rows(yn, 0), pn)

    def weights_c():
        if grid:
            far = o + dx + dy
            w_take(4, rows(far, 0), yn)
            w_copy(11, rows(far, 0), rows(far, 0), pn)
            w_take(5, rows(far, 1), xn)
            w_copy(12, rows(far, 1), rows(far, 1), pn)
            w_take(6, rows(pn), pn)
            w_take(7, rows(pn + dx, 0), pn)
            w_take(8, rows(pn + dy, 1), pn)
            w_take(9, rows(pn + dx, 1), pn)
            w_take(10, rows(pn + dy, 0), pn)
            w_take(11, rows(pn + dx + dy, 0), pn)
            w_take(12, rows(pn + dx + dy, 1), pn)
        else:
            for d in range(1, no):
                w_take(d, rows((o + no - d) % no), (o + no - d) % no)

    def state(b):
        loads[0, b].wait()
        loads[1, b].wait()

        def turn(i, _):
            at = pl.ds(pl.multiple_of(i * TILE, TILE), TILE)
            kf[:, at, :] = jnp.swapaxes(feature_map(kin[b, at]), 0, 1)
            vt[:, at, :] = jnp.swapaxes(vin[b, at], 0, 1)
            return 0

        lax.fori_loop(0, tokens // TILE, turn, 0)

        def head(h, _):
            keys = kf[h]
            part[b, h] = lax.dot_general(
                vt[h], keys, (((0,), (0,)), ((), ())), preferred_element_type=jnp.float32
            )
            mown[b, pl.ds(h, 1), :] = jnp.sum(keys.astype(jnp.float32), axis=0, keepdims=True)
            return 0

        lax.fori_loop(0, heads, head, 0)

    def right_copy(b, n):
        return remote(sr.at[b, n], rr.at[b, n], rr_send.at[b, n], rr_recv.at[b, n], span=(s + 1) % ns)

    def left_copy(b, n):
        return remote(sl.at[b, n], rl.at[b, n], rl_send.at[b, n], rl_recv.at[b, n], span=(s + ns - 1) % ns)

    def term(b, n):
        return part[b, pl.ds(n * chunk, chunk)]

    def sums_start(b):
        @pl.when(s == 0)
        def _():
            for n in range(ns - 1, 0, -1):
                sr[b, n] = term(b, n).astype(jnp.bfloat16)
                right_copy(b, n).start()

        @pl.when(s == ns - 1)
        def _():
            for n in range(ns - 1):
                sl[b, n] = term(b, n).astype(jnp.bfloat16)
                left_copy(b, n).start()

    def sums_middle(b, i):
        to_right, to_left = ns - 1 - i, i

        @pl.when((s > 0) & (s < to_right))
        def _():
            right_copy(b, to_right).wait_recv()
            sr[b, to_right] = (term(b, to_right) + rr[b, to_right].astype(jnp.float32)).astype(jnp.bfloat16)
            right_copy(b, to_right).start()

        @pl.when((s < ns - 1) & (s > to_left))
        def _():
            left_copy(b, to_left).wait_recv()
            sl[b, to_left] = (term(b, to_left) + rl[b, to_left].astype(jnp.float32)).astype(jnp.bfloat16)
            left_copy(b, to_left).start()

    def whole(b, n):
        return full.at[b, pl.ds(n * chunk, chunk)]

    def on_right(b, n):
        return remote(whole(b, n), whole(b, n), ag_sr.at[b, n], ag_recv.at[b, n], span=(s + 1) % ns)

    def on_left(b, n):
        return remote(whole(b, n), whole(b, n), ag_sl.at[b, n], ag_recv.at[b, n], span=(s + ns - 1) % ns)

    def sums_end(b):
        acc[...] = term(b, s)

        @pl.when(s > 0)
        def _():
            right_copy(b, s).wait_recv()
            acc[...] += rr[b, s].astype(jnp.float32)

        @pl.when(s < ns - 1)
        def _():
            left_copy(b, s).wait_recv()
            acc[...] += rl[b, s].astype(jnp.float32)

        full[b, pl.ds(s * chunk, chunk)] = (acc[...] / count).astype(jnp.bfloat16)

        @pl.when(s < ns - 1)
        def _():
            on_right(b, s).start()

        @pl.when(s > 0)
        def _():
            on_left(b, s).start()

    def pass_on(b, d):
        @pl.when(s - d >= 0)
        def _():
            on_right(b, s - d).wait_recv()

            @pl.when(s < ns - 1)
            def _():
                on_right(b, s - d).start()

        @pl.when(s + d <= ns - 1)
        def _():
            on_left(b, s + d).wait_recv()

            @pl.when(s > 0)
            def _():
                on_left(b, s + d).start()

    def mass_copy(d):
        return remote(mown, mrecv.at[d], m_send.at[d], m_recv.at[d], span=(s + d) % ns)

    def ready(b, low, high):
        def turn(i, _):
            at = pl.ds(pl.multiple_of(i * TILE, TILE), TILE)
            qf[b, :, at, :] = jnp.swapaxes(feature_map(qin[b, at]), 0, 1)
            gs[b, :, at, :] = jax.nn.sigmoid(jnp.swapaxes(gin[b, at], 0, 1).astype(jnp.float32))
            return 0

        lax.fori_loop(low, high, turn, 0)

    def read(b):
        def head(h, _):
            row = mown[b, pl.ds(h, 1), :]
            for d in range(1, ns):
                row = row + mrecv[d, b, pl.ds(h, 1), :]
            wide = jnp.broadcast_to(row / count, (size, size))
            high = wide.astype(jnp.bfloat16)
            low = (wide - high.astype(jnp.float32)).astype(jnp.bfloat16)
            top = jnp.concatenate([full[b, h], jnp.zeros((size, size), jnp.bfloat16)], axis=1)
            right = jnp.concatenate([top, jnp.concatenate([high, low], axis=1)], axis=0)
            columns = pl.ds(pl.multiple_of(h * size, size), size)
            for t in range(0, tokens, ROWS):
                f = qf[b, h, t : t + ROWS]
                both = lax.dot_general(
                    jnp.concatenate([f, f], axis=1), right, (((1,), (1,)), ((), ())),
                    preferred_element_type=jnp.float32,
                )
                result = both[:, :size] / (both[:, size:] + 0.001) * count**0.5
                mixed[b, t : t + ROWS, columns] = (result * gs[b, h, t : t + ROWS]).astype(jnp.bfloat16)
            return 0

        lax.fori_loop(0, heads, head, 0)
        copy = pltpu.make_async_copy(mixed.at[b], mixed_hbm.at[b], out_sem.at[b])
        copy.start()
        return copy

    for b in range(batch):
        state(b)
        sums_start(b)
    for d in range(1, ns):
        mass_copy(d).start()
    tiles = tokens // TILE
    for i in range(ns):
        for b in range(batch):
            sums_middle(b, i)
        if i == 1:
            weights_a()
        if i < batch:
            for n in (2, 3):
                loads[n, i].wait()
            ready(i, 0, tiles)
    for b in range(min(ns, batch), batch):
        for n in (2, 3):
            loads[n, b].wait()
        ready(b, 0, tiles)
    for b in range(batch):
        sums_end(b)
    for d in range(1, ns):
        for b in range(batch):
            pass_on(b, d)
    weights_b()
    for d in range(1, ns):
        mass_copy(d).wait_recv()
    stored = [read(b) for b in range(batch)]
    weights_c()

    for copy in stored:
        copy.wait()
    keep_w.wait()
    for copy in sends:
        copy.wait_send()
    for d in range(1, ns):
        mass_copy(d).wait_send()
    for b in range(batch):
        for n in range(ns):

            @pl.when(s < n)
            def _():
                right_copy(b, n).wait_send()

            @pl.when(s > n)
            def _():
                left_copy(b, n).wait_send()

            @pl.when((n <= s) & (s < ns - 1))
            def _():
                on_right(b, n).wait_send()

            @pl.when((n >= s) & (s > 0))
            def _():
                on_left(b, n).wait_send()


def body(queries_in, keys_in, values_in, gate_rows, out_weight):
    batch, tokens, heads, size = queries_in.shape
    depth, width = out_weight.shape
    no, ns = lax.axis_size("outer"), lax.axis_size("span")
    chunk = heads // ns
    bf, f32 = jnp.bfloat16, jnp.float32
    dma = pltpu.SemaphoreType.DMA
    anywhere = pl.BlockSpec(memory_space=pl.ANY)
    copies = max(13, no)
    slots = pltpu.VMEM((batch, ns, chunk, size, size), bf)
    block = pltpu.VMEM((batch, tokens, heads, size), bf)
    mixed, weight = pl.pallas_call(
        functools.partial(kernel, no, ns),
        out_shape=(
            jax.ShapeDtypeStruct((batch, tokens, heads * size), bf),
            jax.ShapeDtypeStruct((no * depth, width), bf),
        ),
        in_specs=[anywhere] * 5,
        out_specs=(anywhere, anywhere),
        scratch_shapes=[
            block, block, block, block,
            pltpu.VMEM((depth, width), bf),
            pltpu.VMEM((heads, tokens, size), bf),
            pltpu.VMEM((heads, tokens, size), bf),
            pltpu.VMEM((batch, heads, tokens, size), bf),
            pltpu.VMEM((batch, heads, tokens, size), f32),
            pltpu.VMEM((batch, heads, size, size), f32),
            pltpu.VMEM((chunk, size, size), f32),
            slots, slots, slots, slots,
            pltpu.VMEM((batch, heads, size, size), bf),
            pltpu.VMEM((batch, heads, size), f32),
            pltpu.VMEM((ns, batch, heads, size), f32),
            pltpu.VMEM((batch, tokens, heads * size), bf),
            dma((4, batch)), dma((2,)), dma((batch,)),
            dma((copies,)), dma((copies,)),
            dma((batch, ns)), dma((batch, ns)), dma((batch, ns)), dma((batch, ns)),
            dma((batch, ns)), dma((batch, ns)), dma((batch, ns)),
            dma((ns,)), dma((ns,)),
        ],
        compiler_params=pltpu.CompilerParams(
            collective_id=0, has_side_effects=True, vmem_limit_bytes=60 * 1024 * 1024
        ),
    )(queries_in, keys_in, values_in, gate_rows, out_weight)
    return jnp.einsum("btw,wv->btv", mixed, weight, preferred_element_type=f32).astype(bf)


def solution(mesh):
    rows = P("outer", "span", None, None)
    in_specs = (rows, rows, rows, rows, P("outer", None))
    out_specs = P("outer", "span", None)
    return jax.shard_map(body, mesh=mesh, in_specs=in_specs, out_specs=out_specs, check_vma=False)
```
